32 devices in a mesh: table: 8 (over y, x, core), batch: 4 (over z).
Axes of the slice: x: 2, y: 2, z: 4, core: 2. Of those that a mesh axis runs over, the one named last changes fastest.
Arguments:
- queries: bfloat16 [128, 4, 512], P(('table', 'batch')), may hold values from -5 to 5
- indices: int32 [128, 4, 32], P(('table', 'batch')), may hold values from 0 to 262143, as said below
- first_keys: bfloat16 [4, 256, 256], P(None, ('table', 'batch')), may hold values from -4 to 4
- second_keys: bfloat16 [4, 1024, 256], replicated, may hold values from -4 to 4
- values: bfloat16 [262144, 1024], P(('table', 'batch')), may hold values from -6 to 6
Outputs:
- memory_read: bfloat16 [128, 1024], P(('table', 'batch'))
The draws below stay inside these ranges and needn't reach their ends.
Inputs may be any that keep to these rules, and one draw needn't show every extreme that they name: `indices`: row r of the value table belongs to device r // 8192 of table+batch. The entries of the 4 sequences of one device name rows of any one owner at most 32 times, and one owner is named exactly 32 times by the entries of every device.
All inputs are finite; a program needn't handle non-finite values.
Results may differ from the reference program's by a relative error of at most 0.005.
Values may be sent and summed in bfloat16 or wider, within the bound.
A program may use at most 64 MiB of HBM per device.

```python
import math
import jax
import jax.numpy as jnp

HEADS = 4
KDIM = 512
HALF = 256
NSUB = 1024
DV = 1024
VALS_DEV = 8192
TOPK = 32
ROWS = 262144
NFIRST = 256
SEQS = 128
ENTRIES = 512
CAP = 32
DEVICES = 32


def owner_table(key):
    base_key = jax.random.fold_in(key, 101)
    hot_owner = jax.random.randint(jax.random.fold_in(base_key, 1), (), 0, DEVICES).astype(jnp.int32)
    others = (hot_owner + 1 + jnp.arange(DEVICES - 1, dtype=jnp.int32)) % DEVICES
    deck_cards = jnp.repeat(others, CAP)
    block_keys = jax.random.split(jax.random.fold_in(base_key, 2), DEVICES)

    def one_block(block_key):
        deal_key, mix_key, row_key = jax.random.split(block_key, 3)
        dealt = jax.random.permutation(deal_key, deck_cards)[:ENTRIES - CAP]
        owners = jnp.concatenate([jnp.zeros((CAP,), jnp.int32) + hot_owner, dealt.astype(jnp.int32)])
        owners = jax.random.permutation(mix_key, owners)
        picked = jax.random.randint(row_key, (ENTRIES,), 0, VALS_DEV).astype(jnp.int32)
        return owners * VALS_DEV + picked
    blocks = jax.vmap(one_block)(block_keys)
    return blocks.reshape(SEQS, HEADS, TOPK).astype(jnp.int32)


def key_table(key, marker, count):
    sub_key = jax.random.fold_in(key, marker)
    drawn = jnp.clip(jax.random.normal(sub_key, (HEADS, count, HALF), jnp.float32), -4.0, 4.0)
    return drawn.astype(jnp.bfloat16)


def draw_indices(key, part):
    return owner_table(key)


def draw_first_keys(key, part):
    return key_table(key, 202, NFIRST)


def draw_second_keys(key, part):
    return key_table(key, 303, NSUB)


def draw_queries(key, part):
    drawn_key = jax.random.fold_in(key, 404)
    spread = 1.4 / math.sqrt(KDIM)
    entries = jnp.clip(jax.random.normal(drawn_key, (SEQS, HEADS, KDIM), jnp.float32), -6.0, 6.0) * spread
    return entries.astype(jnp.bfloat16)


def level_of(stream_key, extent, shards, low, top_value):
    level = 1.0
    for position, blocks in shards:
        draws = jax.random.uniform(jax.random.fold_in(jax.random.fold_in(stream_key, 6), position), (blocks,), jnp.float32, low / len(shards), top_value / len(shards))
        level = level * jnp.repeat(jnp.exp(draws), extent[position] // blocks).reshape((-1,) + (1,) * (len(extent) - 1 - position))
    return level


def noise(own_key, extent, deviation, bound, cuts=(), held_as=jnp.bfloat16):
    values = deviation * jax.random.normal(own_key, extent, jnp.float32)
    if cuts:
        values = values * level_of(own_key, extent, cuts, -0.22, 0.18)
    return jnp.clip(values, -bound, bound).astype(held_as)


def setup_inputs(seed: int = 0) -> dict:
    key_list = jax.random.split(jax.random.key(seed), 6)
    return {
        "queries": draw_queries(jax.random.fold_in(key_list[5], 71), 0),
        "indices": draw_indices(jax.random.fold_in(key_list[5], 71), 0),
        "first_keys": draw_first_keys(jax.random.fold_in(key_list[5], 71), 0),
        "second_keys": draw_second_keys(jax.random.fold_in(key_list[5], 71), 0),
        "values": noise(key_list[4], (ROWS, DV), 1.0, 6.0, ((0, 32),)),
    }


def reference(queries, indices, first_keys, second_keys, values):
    head_ids = jnp.arange(HEADS, dtype=jnp.int32)[None, :, None]
    first_ids = (indices // NSUB).astype(jnp.int32)
    second_ids = (indices % NSUB).astype(jnp.int32)
    query_first = queries[:, :, :HALF].astype(jnp.float32)
    query_second = queries[:, :, HALF:].astype(jnp.float32)
    first_rows = first_keys[head_ids, first_ids].astype(jnp.float32)
    second_rows = second_keys[head_ids, second_ids].astype(jnp.float32)
    first_part = jnp.sum(query_first[:, :, None, :] * first_rows, axis=-1)
    second_part = jnp.sum(query_second[:, :, None, :] * second_rows, axis=-1)
    weights = jax.nn.softmax(first_part + second_part, axis=-1).astype(jnp.bfloat16)
    result = jnp.zeros((SEQS, DV), jnp.float32)
    for head_index in range(HEADS):
        fetched = values[indices[:, head_index]].astype(jnp.float32)
        result = result + jnp.einsum("sk,skd->sd", weights[:, head_index].astype(jnp.float32), fetched)
    return result.astype(jnp.bfloat16)
```

```python
import functools

import jax
import jax.numpy as jnp
from jax import lax
from jax.experimental import pallas as pl
from jax.experimental.pallas import tpu as pltpu
from jax.sharding import PartitionSpec as P

MESH = pl.DeviceIdType.MESH
LANES = 128
NT = (((1,), (1,)), ((), ()))


def log2(number):
    assert number & (number - 1) == 0
    return number.bit_length() - 1


def pick_lanes(table, ids):
    picked = jnp.zeros(ids.shape, jnp.float32)
    inner = ids & (LANES - 1)
    outer = lax.shift_right_arithmetic(ids, 7)
    for part in range(table.shape[1] // LANES):
        got = jnp.take_along_axis(table[:, part * LANES : (part + 1) * LANES], inner, axis=1)
        picked = jnp.where(outer == part, got, picked)
    return picked


def kernel(
    shape,
    q_ref,
    i_ref,
    fk_ref,
    sk_ref,
    v_ref,
    out_ref,
    vbuf,
    k2buf,
    kslot,
    islot,
    icomp,
    qslot,
    qrows,
    grows,
    rolled,
    wpack,
    wslot,
    istage,
    wstage,
    wfin,
    wacc,
    wb,
    psend,
    pslot,
    v_sem,
    k2_sem,
    k_send,
    k_recv,
    i_send,
    i_recv,
    q_send,
    q_recv,
    w_send,
    w_recv,
    p_send,
    p_recv,
):
    nt, nb, heads, seqs, top, chunks, pieces = shape
    devices = nt * nb
    groups = devices // heads
    half = q_ref.shape[2] // 2
    rows, width = v_ref.shape
    t_me, b_me = lax.axis_index("table"), lax.axis_index("batch")
    dev_me = t_me * nb + b_me
    head_me = lax.rem(t_me, heads)
    group_me = lax.div(t_me, heads) * nb + b_me
    slot_me = head_me * groups + group_me

    def place(slot):
        head = lax.div(slot, groups)
        group = lax.rem(slot, groups)
        return lax.div(group, nb) * heads + head, lax.rem(group, nb), head

    def others(body):
        def step(offset, carry):
            slot = lax.rem(slot_me + offset, devices)
            t, b, head = place(slot)
            body(slot, (t, b), head)
            return carry

        lax.fori_loop(1, devices, step, 0)

    def drain(ref, sem):
        pltpu.make_async_copy(ref, ref, sem).wait()

    k2_copy = pltpu.make_async_copy(sk_ref.at[head_me], k2buf, k2_sem)
    k2_copy.start()
    block = rows // pieces
    v_copies = [
        pltpu.make_async_copy(
            v_ref.at[pl.ds(p * block, block)], vbuf.at[pl.ds(p * block, block)], v_sem.at[p]
        )
        for p in range(pieces)
    ]
    for copy in v_copies:
        copy.start()

    barrier = pltpu.get_barrier_semaphore()
    others(
        lambda slot, where, head: pl.semaphore_signal(
            barrier, inc=1, device_id=where, device_id_type=MESH
        )
    )
    for h in range(heads):
        for s in range(seqs):
            icomp[pl.ds(s, 1), pl.ds(h * top, top)] = i_ref[s, pl.ds(h, 1), :]
    islot[slot_me] = icomp[...]
    kslot[dev_me] = fk_ref[head_me]
    qslot[head_me] = q_ref[...]
    pl.semaphore_wait(barrier, devices - 1)

    def send_q(j):
        other = lax.rem(head_me + j, heads)
        pltpu.make_async_remote_copy(
            src_ref=q_ref,
            dst_ref=qslot.at[head_me],
            send_sem=q_send,
            recv_sem=q_recv,
            device_id=(lax.div(t_me, heads) * heads + other, b_me),
            device_id_type=MESH,
        ).start()

    for j in range(1, heads):
        send_q(j)

    def send_keys(slot, where, head):
        pltpu.make_async_remote_copy(
            src_ref=fk_ref.at[head],
            dst_ref=kslot.at[dev_me],
            send_sem=k_send,
            recv_sem=k_recv,
            device_id=where,
            device_id_type=MESH,
        ).start()

    def send_ids(slot, where, head):
        pltpu.make_async_remote_copy(
            src_ref=icomp,
            dst_ref=islot.at[slot_me],
            send_sem=i_send,
            recv_sem=i_recv,
            device_id=where,
            device_id_type=MESH,
        ).start()

    others(send_keys)
    others(send_ids)

    drain(qslot.at[pl.ds(0, heads - 1)], q_recv)
    for j in range(heads):
        for s in range(seqs):
            one = qslot[j, s].astype(jnp.float32)
            for c in range(qrows.shape[0]):
                qrows[c, pl.ds((j * seqs + s) * heads, heads), :] = one[
                    :, c * LANES : (c + 1) * LANES
                ]
    q_all = jnp.concatenate(
        [
            qrows.at[c][pl.ds(head_me, heads * seqs, stride=heads), :]
            for c in range(qrows.shape[0])
        ],
        axis=1,
    ).astype(jnp.bfloat16)
    k2_copy.wait()
    s2 = lax.dot_general(q_all[:, half:], k2buf[...], NT, preferred_element_type=jnp.float32)
    drain(islot.at[pl.ds(0, devices - 1)], i_recv)
    for j in range(heads):
        grows[pl.ds(j * seqs, seqs), :] = islot[j * groups + group_me]
    ids = grows[...]
    sub_count = k2buf.shape[0]
    second = pick_lanes(s2, ids & (sub_count - 1))
    for slot in range(devices):
        istage[pl.ds(slot * seqs, seqs), :] = islot[slot]
    drain(kslot.at[pl.ds(0, devices - 1)], k_recv)
    k1 = kslot[...].astype(jnp.float32)
    k1 = k1.reshape(k1.shape[0] * k1.shape[1], half).astype(jnp.bfloat16)
    s1 = lax.dot_general(q_all[:, :half], k1, NT, preferred_element_type=jnp.float32)
    score = second + pick_lanes(s1, lax.shift_right_arithmetic(ids, log2(sub_count)))
    lane = lax.broadcasted_iota(jnp.int32, ids.shape, 1)
    mine = lax.shift_right_arithmetic(lane, log2(top)) == head_me
    best = jnp.max(jnp.where(mine, score, -jnp.inf), axis=1, keepdims=True)
    raised = jnp.where(mine, jnp.exp(jnp.where(mine, score - best, 0.0)), 0.0)
    weights = raised / jnp.sum(raised, axis=1, keepdims=True)
    weights = weights.astype(jnp.bfloat16).astype(jnp.float32)
    for j in range(heads):
        rolled[j] = pltpu.roll(weights, lax.rem(j - head_me + heads, heads) * top, 1)
    packed = rolled[0, pl.ds(0, seqs), :]
    for j in range(1, heads):
        packed = packed + rolled[j, pl.ds(j * seqs, seqs), :]
    wpack[...] = packed
    wslot[slot_me] = packed

    def send_weights(slot, where, head):
        pltpu.make_async_remote_copy(
            src_ref=wpack,
            dst_ref=wslot.at[slot_me],
            send_sem=w_send,
            recv_sem=w_recv,
            device_id=where,
            device_id_type=MESH,
        ).start()

    others(send_weights)
    drain(wslot.at[pl.ds(0, devices - 1)], w_recv)
    for slot in range(devices):
        wstage[pl.ds(slot * seqs, seqs), :] = wslot[slot]
    span = groups * seqs
    lane = lax.broadcasted_iota(jnp.int32, (span, LANES), 1)
    block_of = lax.shift_right_arithmetic(lane, log2(top))
    for j in range(heads):
        total = jnp.zeros((span, LANES), jnp.float32)
        for h in range(heads):
            part = wstage[pl.ds(h * span, span), :]
            if h != j:
                part = pltpu.roll(part, (h - j) % heads * top, 1)
            total = jnp.where(block_of == h, part, total)
        wfin[pl.ds(j * span, span), :] = total

    high_count = rows // LANES
    all_seqs = devices * seqs
    high_iota = lax.broadcasted_iota(jnp.int32, (high_count, LANES), 0)
    low_iota = lax.broadcasted_iota(jnp.int32, (LANES, LANES), 0)
    base = dev_me * rows

    def spread(step, carry):
        for u in range(8):
            s = step * 8 + u
            row = istage[pl.ds(s, 1), :]
            high = lax.shift_right_arithmetic(row - base, 7)
            low = row & (LANES - 1)
            left = jnp.where(high_iota == high, wfin[pl.ds(s, 1), :], 0.0).astype(jnp.bfloat16)
            right = jnp.where(low_iota == low, 1.0, 0.0).astype(jnp.bfloat16)
            wacc[pl.ds(s, high_count, stride=all_seqs), :] = lax.dot_general(
                left, right, NT, preferred_element_type=jnp.float32
            )
        return carry

    lax.fori_loop(0, all_seqs // 8, spread, 0)

    def narrow(step, carry):
        wb[:, pl.ds(pl.multiple_of(step * LANES, LANES), LANES)] = wacc[
            pl.ds(pl.multiple_of(step * all_seqs, all_seqs), all_seqs), :
        ].astype(jnp.bfloat16)
        return carry

    lax.fori_loop(0, high_count, narrow, 0)
    for copy in v_copies:
        copy.wait()

    piece = width // chunks
    deep = min(1024, rows)
    for c in range(chunks):

        def multiply(step, acc):
            at = pl.multiple_of(step * deep, deep)
            return acc + jnp.dot(
                wb[:, pl.ds(at, deep)],
                vbuf[pl.ds(at, deep), pl.ds(c * piece, piece)],
                preferred_element_type=jnp.float32,
            )

        acc = lax.fori_loop(
            0, rows // deep, multiply, jnp.zeros((all_seqs, piece), jnp.float32)
        )
        for slot in range(devices):
            psend[c, slot] = acc[slot * seqs : (slot + 1) * seqs, :].astype(jnp.bfloat16)
        pslot[c, slot_me] = psend[c, slot_me]

        def send_part(slot, where, head):
            pltpu.make_async_remote_copy(
                src_ref=psend.at[c, slot],
                dst_ref=pslot.at[c, slot_me],
                send_sem=p_send.at[c],
                recv_sem=p_recv.at[c],
                device_id=where,
                device_id_type=MESH,
            ).start()

        others(send_part)

    for c in range(chunks):
        drain(pslot.at[c, pl.ds(0, devices - 1)], p_recv.at[c])
        total = jnp.zeros((seqs, piece), jnp.float32)
        for slot in range(devices):
            total = total + pslot[c, slot].astype(jnp.float32)
        out_ref[:, pl.ds(c * piece, piece)] = total.astype(jnp.bfloat16)

    drain(qslot.at[pl.ds(0, heads - 1)], q_send)
    drain(kslot.at[pl.ds(0, devices - 1)], k_send)
    drain(islot.at[pl.ds(0, devices - 1)], i_send)
    drain(wslot.at[pl.ds(0, devices - 1)], w_send)
    for c in range(chunks):
        drain(pslot.at[c, pl.ds(0, devices - 1)], p_send.at[c])


def shards(nt, nb, queries, indices, first_keys, second_keys, values):
    seqs, heads, top = indices.shape
    width_q = queries.shape[2]
    half = width_q // 2
    firsts = first_keys.shape[1]
    sub_count = second_keys.shape[1]
    rows, width = values.shape
    devices = nt * nb
    all_seqs = devices * seqs
    assert heads * top == LANES and nt % heads == 0
    chunks, pieces = 4, 4
    vmem = pl.BlockSpec(memory_space=pltpu.VMEM)
    hbm = pl.BlockSpec(memory_space=pl.ANY)
    dma = pltpu.SemaphoreType.DMA
    return pl.pallas_call(
        functools.partial(kernel, (nt, nb, heads, seqs, top, chunks, pieces)),
        out_shape=jax.ShapeDtypeStruct((seqs, width), jnp.bfloat16),
        in_specs=[vmem, vmem, vmem, hbm, hbm],
        out_specs=vmem,
        scratch_shapes=[
            pltpu.VMEM((rows, width), jnp.bfloat16),
            pltpu.VMEM((sub_count, half), jnp.bfloat16),
            pltpu.VMEM((devices, firsts, half), jnp.bfloat16),
            pltpu.VMEM((devices, seqs, LANES), jnp.int32),
            pltpu.VMEM((seqs, LANES), jnp.int32),
            pltpu.VMEM((heads, seqs, heads, width_q), jnp.bfloat16),
            pltpu.VMEM((width_q // LANES, heads * seqs * heads, LANES), jnp.float32),
            pltpu.VMEM((heads * seqs, LANES), jnp.int32),
            pltpu.VMEM((heads, heads * seqs, LANES), jnp.float32),
            pltpu.VMEM((seqs, LANES), jnp.float32),
            pltpu.VMEM((devices, seqs, LANES), jnp.float32),
            pltpu.VMEM((all_seqs, LANES), jnp.int32),
            pltpu.VMEM((all_seqs, LANES), jnp.float32),
            pltpu.VMEM((all_seqs, LANES), jnp.float32),
            pltpu.VMEM((rows // LANES * all_seqs, LANES), jnp.float32),
            pltpu.VMEM((all_seqs, rows), jnp.bfloat16),
            pltpu.VMEM((chunks, devices, seqs, width // chunks), jnp.bfloat16),
            pltpu.VMEM((chunks, devices, seqs, width // chunks), jnp.bfloat16),
            dma((pieces,)),
            dma,
            dma,
            dma,
            dma,
            dma,
            dma,
            dma,
            dma,
            dma,
            dma((chunks,)),
            dma((chunks,)),
        ],
        compiler_params=pltpu.CompilerParams(
            collective_id=0, has_side_effects=True, vmem_limit_bytes=60 * 1024 * 1024
        ),
    )(queries, indices, first_keys, second_keys, values)


def solution(mesh):
    placed = (
        P(("table", "batch"), None, None),
        P(("table", "batch"), None, None),
        P(None, ("table", "batch"), None),
        P(),
        P(("table", "batch"), None),
    )
    body = functools.partial(shards, mesh.shape["table"], mesh.shape["batch"])
    return jax.shard_map(
        body, mesh=mesh, in_specs=placed, out_specs=P(("table", "batch"), None), check_vma=False
    )
```

```python
import functools

import jax
import jax.numpy as jnp
from jax import lax
from jax.experimental import pallas as pl
from jax.experimental.pallas import tpu as pltpu
from jax.sharding import PartitionSpec as P

MESH = pl.DeviceIdType.MESH
LANES = 128
NT = (((1,), (1,)), ((), ()))
NN = (((1,), (0,)), ((), ()))


def log2(number):
    assert number & (number - 1) == 0
    return number.bit_length() - 1


def pick_lanes(table, ids):
    picked = jnp.zeros(ids.shape, jnp.float32)
    inner = ids & (LANES - 1)
    outer = lax.shift_right_arithmetic(ids, 7)
    for part in range(table.shape[1] // LANES):
        got = jnp.take_along_axis(table[:, part * LANES : (part + 1) * LANES], inner, axis=1)
        picked = jnp.where(outer == part, got, picked)
    return picked


def kernel(
    shape,
    q_ref,
    i_ref,
    fk_ref,
    sk_ref,
    v_ref,
    out_ref,
    vbuf,
    k2buf,
    kslot,
    islot,
    gslot,
    icomp,
    qslot,
    qrows,
    grows,
    rolled,
    wpack,
    wslot,
    istage,
    wstage,
    wfin,
    wacc,
    wb,
    lows,
    accs,
    pair,
    psend,
    pslot,
    v_sem,
    k2_sem,
    k_send,
    k_recv,
    i_send,
    i_recv,
    g_send,
    g_recv,
    q_send,
    q_recv,
    w_send,
    w_recv,
    a_send,
    a_recv,
    p_send,
    p_recv,
):
    nt, nb, heads, seqs, top, chunks, pieces, early = shape
    devices = nt * nb
    groups = devices // heads
    half = q_ref.shape[2] // 2
    rows, width = v_ref.shape
    t_me, b_me = lax.axis_index("table"), lax.axis_index("batch")
    dev_me = t_me * nb + b_me
    head_me = lax.rem(t_me, heads)
    group_me = lax.div(t_me, heads) * nb + b_me
    slot_me = head_me * groups + group_me

    def others(body, stride=1):
        def visit(shift, first):
            t = lax.rem(t_me + shift * stride, nt)
            head = lax.rem(t, heads)
            start = head * groups + lax.div(t, heads) * nb
            for k in range(first, nb):
                b = lax.rem(b_me + k, nb)
                body(start + b, (t, b), head)

        def step(shift, carry):
            visit(shift, 0)
            return carry

        visit(0, 1)
        lax.fori_loop(1, nt // stride, step, 0)

    def drain(ref, sem):
        pltpu.make_async_copy(ref, ref, sem).wait()

    k2_copy = pltpu.make_async_copy(sk_ref.at[head_me], k2buf, k2_sem)
    k2_copy.start()
    block = rows // pieces
    v_copies = [
        pltpu.make_async_copy(
            v_ref.at[pl.ds(p * block, block)], vbuf.at[pl.ds(p * block, block)], v_sem.at[p]
        )
        for p in range(pieces)
    ]
    for copy in v_copies:
        copy.start()

    barrier = pltpu.get_barrier_semaphore()
    others(
        lambda slot, where, head: pl.semaphore_signal(
            barrier, inc=1, device_id=where, device_id_type=MESH
        )
    )
    for h in range(heads):
        for s in range(seqs):
            icomp[pl.ds(s, 1), pl.ds(h * top, top)] = i_ref[s, pl.ds(h, 1), :]
    islot[slot_me] = icomp[...]
    kslot[dev_me] = fk_ref[head_me]
    gslot[head_me] = icomp[...]
    qslot[head_me] = q_ref[...]
    pl.semaphore_wait(barrier, devices - 1)

    def send_q(j):
        other = lax.rem(head_me + j, heads)
        pltpu.make_async_remote_copy(
            src_ref=q_ref,
            dst_ref=qslot.at[head_me],
            send_sem=q_send,
            recv_sem=q_recv,
            device_id=(lax.div(t_me, heads) * heads + other, b_me),
            device_id_type=MESH,
        ).start()

    def send_group_ids(j):
        other = lax.rem(head_me + j, heads)
        pltpu.make_async_remote_copy(
            src_ref=icomp,
            dst_ref=gslot.at[head_me],
            send_sem=g_send,
            recv_sem=g_recv,
            device_id=(lax.div(t_me, heads) * heads + other, b_me),
            device_id_type=MESH,
        ).start()

    for j in range(1, heads):
        send_q(j)
        send_group_ids(j)

    def send_keys(slot, where, head):
        pltpu.make_async_remote_copy(
            src_ref=fk_ref.at[head],
            dst_ref=kslot.at[dev_me],
            send_sem=k_send,
            recv_sem=k_recv,
            device_id=where,
            device_id_type=MESH,
        ).start()

    def send_ids(slot, where, head):
        pltpu.make_async_remote_copy(
            src_ref=icomp,
            dst_ref=islot.at[slot_me],
            send_sem=i_send,
            recv_sem=i_recv,
            device_id=where,
            device_id_type=MESH,
        ).start()

    others(send_keys)
    others(send_ids)

    drain(qslot.at[pl.ds(0, heads - 1)], q_recv)
    for j in range(heads):
        for s in range(seqs):
            one = qslot[j, s].astype(jnp.float32)
            for c in range(qrows.shape[0]):
                qrows[c, pl.ds((j * seqs + s) * heads, heads), :] = one[
                    :, c * LANES : (c + 1) * LANES
                ]
    q_all = jnp.concatenate(
        [
            qrows.at[c][pl.ds(head_me, heads * seqs, stride=heads), :]
            for c in range(qrows.shape[0])
        ],
        axis=1,
    ).astype(jnp.bfloat16)
    k2_copy.wait()
    s2 = lax.dot_general(q_all[:, half:], k2buf[...], NT, preferred_element_type=jnp.float32)
    drain(gslot.at[pl.ds(0, heads - 1)], g_recv)
    for j in range(heads):
        grows[pl.ds(j * seqs, seqs), :] = gslot[j]
    ids = grows[...]
    sub_count = k2buf.shape[0]
    second = pick_lanes(s2, ids & (sub_count - 1))
    drain(kslot.at[pl.ds(0, devices - 1)], k_recv)
    k1 = kslot[...].astype(jnp.float32)
    k1 = k1.reshape(k1.shape[0] * k1.shape[1], half).astype(jnp.bfloat16)
    s1 = lax.dot_general(q_all[:, :half], k1, NT, preferred_element_type=jnp.float32)
    score = second + pick_lanes(s1, lax.shift_right_arithmetic(ids, log2(sub_count)))
    lane = lax.broadcasted_iota(jnp.int32, ids.shape, 1)
    mine = lax.shift_right_arithmetic(lane, log2(top)) == head_me
    best = jnp.max(jnp.where(mine, score, -jnp.inf), axis=1, keepdims=True)
    raised = jnp.where(mine, jnp.exp(jnp.where(mine, score - best, 0.0)), 0.0)
    weights = raised / jnp.sum(raised, axis=1, keepdims=True)
    weights = weights.astype(jnp.bfloat16).astype(jnp.float32)
    for j in range(heads):
        rolled[j] = pltpu.roll(weights, lax.rem(j - head_me + heads, heads) * top, 1)
    packed = rolled[0, pl.ds(0, seqs), :]
    for j in range(1, heads):
        packed = packed + rolled[j, pl.ds(j * seqs, seqs), :]
    wpack[...] = packed
    wslot[slot_me] = packed

    def send_weights(slot, where, head):
        pltpu.make_async_remote_copy(
            src_ref=wpack,
            dst_ref=wslot.at[slot_me],
            send_sem=w_send,
            recv_sem=w_recv,
            device_id=where,
            device_id_type=MESH,
        ).start()

    others(send_weights)
    high_count = rows // LANES
    all_seqs = devices * seqs
    high_iota = lax.broadcasted_iota(jnp.int32, (high_count, LANES), 0)
    low_iota = lax.broadcasted_iota(jnp.int32, (LANES, LANES), 0)
    base = dev_me * rows

    def high_hot(s, value):
        high = lax.shift_right_arithmetic(istage[pl.ds(s, 1), :] - base, 7)
        return jnp.where(high_iota == high, value, 0.0).astype(jnp.bfloat16)

    def low_hot(s):
        low = istage[pl.ds(s, 1), :] & (LANES - 1)
        return jnp.where(low_iota == low, 1.0, 0.0).astype(jnp.bfloat16)

    drain(islot.at[pl.ds(0, devices - 1)], i_recv)
    for slot in range(devices):
        istage[pl.ds(slot * seqs, seqs), :] = islot[slot]
    low_lane = lax.broadcasted_iota(jnp.int32, (LANES, LANES), 1).astype(jnp.float32)
    if early:

        def build(step, carry):
            some = istage[pl.ds(pl.multiple_of(step * 8, 8), 8), :] & (LANES - 1)
            some = some.astype(jnp.float32).T
            for u in range(8):
                hot = jnp.where(low_lane == some[:, u : u + 1], 1.0, 0.0)
                lows[step * 8 + u] = hot.astype(jnp.bfloat16)
            return carry

        lax.fori_loop(0, all_seqs // 8, build, 0)
    drain(wslot.at[pl.ds(0, devices - 1)], w_recv)
    for slot in range(devices):
        wstage[pl.ds(slot * seqs, seqs), :] = wslot[slot]
    span = groups * seqs
    lane = lax.broadcasted_iota(jnp.int32, (span, LANES), 1)
    block_of = lax.shift_right_arithmetic(lane, log2(top))
    for j in range(heads):
        total = jnp.zeros((span, LANES), jnp.float32)
        for h in range(heads):
            part = wstage[pl.ds(h * span, span), :]
            if h != j:
                part = pltpu.roll(part, (h - j) % heads * top, 1)
            total = jnp.where(block_of == h, part, total)
        wfin[pl.ds(j * span, span), :] = total

    pitch = all_seqs + 8

    def spread(step, carry):
        for u in range(32):
            s = step * 32 + u
            left = high_hot(s, wfin[pl.ds(s, 1), :])
            right = lows[s] if early else low_hot(s)
            wacc[pl.ds(s, high_count, stride=pitch), :] = lax.dot_general(
                left, right, NN if early else NT, preferred_element_type=jnp.float32
            )
        return carry

    lax.fori_loop(0, all_seqs // 32, spread, 0)

    def narrow(step, carry):
        wb[:, pl.ds(pl.multiple_of(step * LANES, LANES), LANES)] = wacc[
            pl.ds(pl.multiple_of(step * pitch, 8), all_seqs), :
        ].astype(jnp.bfloat16)
        return carry

    lax.fori_loop(0, high_count, narrow, 0, unroll=8)
    for copy in v_copies:
        copy.wait()

    piece = width // chunks
    core_me = lax.rem(t_me, 2)
    half_slot = lax.div(head_me, 2) * groups + group_me

    def pass_on(c):
        drain(pair.at[c], a_recv.at[c])
        for i in range(heads // 2):
            both = accs[c, 2 * i + core_me] + pair[c, i]
            for g in range(groups):
                psend[c, i * groups + g] = both[g * seqs : (g + 1) * seqs, :].astype(jnp.bfloat16)
        pslot[c, half_slot] = psend[c, half_slot]

        def send_part(slot, where, head):
            pltpu.make_async_remote_copy(
                src_ref=psend.at[c, slot - lax.div(head + 1, 2) * groups],
                dst_ref=pslot.at[c, half_slot],
                send_sem=p_send.at[c],
                recv_sem=p_recv.at[c],
                device_id=where,
                device_id_type=MESH,
            ).start()

        others(send_part, 2)

    for c in range(chunks):
        acc = jnp.dot(
            wb[...], vbuf[:, pl.ds(c * piece, piece)], preferred_element_type=jnp.float32
        )
        for j in range(heads):
            accs[c, j] = acc[j * span : (j + 1) * span, :]
        for i in range(heads // 2):
            pltpu.make_async_remote_copy(
                src_ref=accs.at[c, 2 * i + 1 - core_me],
                dst_ref=pair.at[c, i],
                send_sem=a_send.at[c],
                recv_sem=a_recv.at[c],
                device_id=(t_me + 1 - 2 * core_me, b_me),
                device_id_type=MESH,
            ).start()
        if c > 0:
            pass_on(c - 1)
    pass_on(chunks - 1)

    for c in range(chunks):
        drain(pslot.at[c, pl.ds(0, devices // 2 - 1)], p_recv.at[c])
        total = jnp.zeros((seqs, piece), jnp.float32)
        for slot in range(devices // 2):
            total = total + pslot[c, slot].astype(jnp.float32)
        out_ref[:, pl.ds(c * piece, piece)] = total.astype(jnp.bfloat16)

    drain(qslot.at[pl.ds(0, heads - 1)], q_send)
    drain(gslot.at[pl.ds(0, heads - 1)], g_send)
    drain(kslot.at[pl.ds(0, devices - 1)], k_send)
    drain(islot.at[pl.ds(0, devices - 1)], i_send)
    drain(wslot.at[pl.ds(0, devices - 1)], w_send)
    for c in range(chunks):
        drain(pslot.at[c, pl.ds(0, devices // 2 - 1)], p_send.at[c])
        drain(pair.at[c], a_send.at[c])


def shards(nt, nb, queries, indices, first_keys, second_keys, values):
    seqs, heads, top = indices.shape
    width_q = queries.shape[2]
    half = width_q // 2
    firsts = first_keys.shape[1]
    sub_count = second_keys.shape[1]
    rows, width = values.shape
    devices = nt * nb
    all_seqs = devices * seqs
    assert heads * top == LANES and nt % heads == 0 and heads % 2 == 0
    chunks, pieces = 2, 4
    early = all_seqs <= 256
    vmem = pl.BlockSpec(memory_space=pltpu.VMEM)
    hbm = pl.BlockSpec(memory_space=pl.ANY)
    dma = pltpu.SemaphoreType.DMA
    return pl.pallas_call(
        functools.partial(kernel, (nt, nb, heads, seqs, top, chunks, pieces, early)),
        out_shape=jax.ShapeDtypeStruct((seqs, width), jnp.bfloat16),
        in_specs=[vmem, vmem, vmem, hbm, hbm],
        out_specs=vmem,
        scratch_shapes=[
            pltpu.VMEM((rows, width), jnp.bfloat16),
            pltpu.VMEM((sub_count, half), jnp.bfloat16),
            pltpu.VMEM((devices, firsts, half), jnp.bfloat16),
            pltpu.VMEM((devices, seqs, LANES), jnp.int32),
            pltpu.VMEM((heads, seqs, LANES), jnp.int32),
            pltpu.VMEM((seqs, LANES), jnp.int32),
            pltpu.VMEM((heads, seqs, heads, width_q), jnp.bfloat16),
            pltpu.VMEM((width_q // LANES, heads * seqs * heads, LANES), jnp.float32),
            pltpu.VMEM((heads * seqs, LANES), jnp.int32),
            pltpu.VMEM((heads, heads * seqs, LANES), jnp.float32),
            pltpu.VMEM((seqs, LANES), jnp.float32),
            pltpu.VMEM((devices, seqs, LANES), jnp.float32),
            pltpu.VMEM((all_seqs, LANES), jnp.int32),
            pltpu.VMEM((all_seqs, LANES), jnp.float32),
            pltpu.VMEM((all_seqs, LANES), jnp.float32),
            pltpu.VMEM((rows // LANES * (all_seqs + 8), LANES), jnp.float32),
            pltpu.VMEM((all_seqs, rows), jnp.bfloat16),
            pltpu.VMEM((all_seqs if early else 1, LANES, LANES), jnp.bfloat16),
            pltpu.VMEM((chunks, heads, all_seqs // heads, width // chunks), jnp.float32),
            pltpu.VMEM((chunks, heads // 2, all_seqs // heads, width // chunks), jnp.float32),
            pltpu.VMEM((chunks, devices // 2, seqs, width // chunks), jnp.bfloat16),
            pltpu.VMEM((chunks, devices // 2, seqs, width // chunks), jnp.bfloat16),
            dma((pieces,)),
            dma,
            dma,
            dma,
            dma,
            dma,
            dma,
            dma,
            dma,
            dma,
            dma,
            dma,
            dma((chunks,)),
            dma((chunks,)),
            dma((chunks,)),
            dma((chunks,)),
        ],
        compiler_params=pltpu.CompilerParams(
            collective_id=0, has_side_effects=True, vmem_limit_bytes=60 * 1024 * 1024
        ),
    )(queries, indices, first_keys, second_keys, values)


def solution(mesh):
    placed = (
        P(("table", "batch"), None, None),
        P(("table", "batch"), None, None),
        P(None, ("table", "batch"), None),
        P(),
        P(("table", "batch"), None),
    )
    body = functools.partial(shards, mesh.shape["table"], mesh.shape["batch"])
    return jax.shard_map(
        body, mesh=mesh, in_specs=placed, out_specs=P(("table", "batch"), None), check_vma=False
    )
```

```python
import functools

import jax
import jax.numpy as jnp
from jax import lax
from jax.experimental import pallas as pl
from jax.experimental.pallas import tpu as pltpu
from jax.sharding import PartitionSpec as P

MESH = pl.DeviceIdType.MESH
LANES = 128
NT = (((1,), (1,)), ((), ()))
NN = (((1,), (0,)), ((), ()))


def log2(number):
    assert number & (number - 1) == 0
    return number.bit_length() - 1


def pick_lanes(table, ids):
    picked = jnp.zeros(ids.shape, jnp.float32)
    inner = ids & (LANES - 1)
    outer = lax.shift_right_arithmetic(ids, 7)
    for part in range(table.shape[1] // LANES):
        got = jnp.take_along_axis(table[:, part * LANES : (part + 1) * LANES], inner, axis=1)
        picked = jnp.where(outer == part, got, picked)
    return picked


def kernel(
    shape,
    q_ref,
    i_ref,
    fk_ref,
    sk_ref,
    v_ref,
    out_ref,
    vbuf,
    k2buf,
    kslot,
    islot,
    gslot,
    icomp,
    qslot,
    qrows,
    grows,
    rolled,
    wpack,
    wslot,
    istage,
    wstage,
    wfin,
    wacc,
    wb,
    lows,
    accs,
    pair,
    psend,
    pslot,
    v_sem,
    k2_sem,
    k_send,
    k_recv,
    i_send,
    i_recv,
    r_send,
    r_recv,
    g_send,
    g_recv,
    q_send,
    q_recv,
    w_send,
    w_recv,
    a_send,
    a_recv,
    p_send,
    p_recv,
):
    nt, nb, heads, seqs, top, chunks, pieces, early = shape
    devices = nt * nb
    groups = devices // heads
    half = q_ref.shape[2] // 2
    rows, width = v_ref.shape
    t_me, b_me = lax.axis_index("table"), lax.axis_index("batch")
    dev_me = t_me * nb + b_me
    core_me = lax.rem(t_me, 2)
    head_me = lax.rem(t_me, heads)
    group_me = lax.div(t_me, heads) * nb + b_me
    slot_me = head_me * groups + group_me

    def flips(x, count):
        bits = [(x // 2**i) % 2 for i in range(log2(count))]
        return [
            x + sum((1 - 2 * bit) * 2**i for i, bit in enumerate(bits) if mask >> i & 1)
            for mask in range(count)
        ]

    t_flips, b_flips = flips(t_me, nt), flips(b_me, nb)
    t_heads = [lax.rem(t, heads) for t in t_flips]
    t_slots = [h * groups + lax.div(t, heads) * nb for t, h in zip(t_flips, t_heads)]
    masks = sorted(
        ((mt, mb) for mt in range(nt) for mb in range(nb) if mt or mb),
        key=lambda m: (m[1] + bin(m[0] >> 1).count("1"), m),
        reverse=True,
    )

    def others(body, stride=1):
        for mt, mb in masks:
            if mt % stride == 0:
                body(t_slots[mt] + b_flips[mb], (t_flips[mt], b_flips[mb]), t_heads[mt])

    def drain(ref, sem):
        pltpu.make_async_copy(ref, ref, sem).wait()

    k2_copy = pltpu.make_async_copy(sk_ref.at[head_me], k2buf, k2_sem)
    k2_copy.start()
    block = rows // pieces
    v_copies = [
        pltpu.make_async_copy(
            v_ref.at[pl.ds(p * block, block)], vbuf.at[pl.ds(p * block, block)], v_sem.at[p]
        )
        for p in range(pieces)
    ]
    for copy in v_copies:
        copy.start()

    barrier = pltpu.get_barrier_semaphore()
    others(
        lambda slot, where, head: pl.semaphore_signal(
            barrier, inc=1, device_id=where, device_id_type=MESH
        )
    )
    for h in range(heads):
        for s in range(seqs):
            icomp[pl.ds(s, 1), pl.ds(h * top, top)] = i_ref[s, pl.ds(h, 1), :]
    islot[slot_me] = icomp[...]
    kslot[dev_me] = fk_ref[head_me]
    gslot[head_me] = icomp[...]
    qslot[head_me] = q_ref[...]
    pl.semaphore_wait(barrier, devices - 1)

    def send_q(j):
        other = lax.rem(head_me + j, heads)
        pltpu.make_async_remote_copy(
            src_ref=q_ref,
            dst_ref=qslot.at[head_me],
            send_sem=q_send,
            recv_sem=q_recv,
            device_id=(lax.div(t_me, heads) * heads + other, b_me),
            device_id_type=MESH,
        ).start()

    def send_group_ids(j):
        other = lax.rem(head_me + j, heads)
        pltpu.make_async_remote_copy(
            src_ref=icomp,
            dst_ref=gslot.at[head_me],
            send_sem=g_send,
            recv_sem=g_recv,
            device_id=(lax.div(t_me, heads) * heads + other, b_me),
            device_id_type=MESH,
        ).start()

    for j in range(1, heads):
        send_q(j)
        send_group_ids(j)

    def send_keys(slot, where, head):
        pltpu.make_async_remote_copy(
            src_ref=fk_ref.at[head],
            dst_ref=kslot.at[dev_me],
            send_sem=k_send,
            recv_sem=k_recv,
            device_id=where,
            device_id_type=MESH,
        ).start()

    def send_ids(slot, where, head):
        pltpu.make_async_remote_copy(
            src_ref=icomp,
            dst_ref=islot.at[slot_me],
            send_sem=i_send,
            recv_sem=i_recv,
            device_id=where,
            device_id_type=MESH,
        ).start()

    others(send_keys)
    others(send_ids)

    drain(qslot.at[pl.ds(0, heads - 1)], q_recv)
    for j in range(heads):
        for s in range(seqs):
            one = qslot[j, s].astype(jnp.float32)
            for c in range(qrows.shape[0]):
                qrows[c, pl.ds((j * seqs + s) * heads, heads), :] = one[
                    :, c * LANES : (c + 1) * LANES
                ]
    q_all = jnp.concatenate(
        [
            qrows.at[c][pl.ds(head_me, heads * seqs, stride=heads), :]
            for c in range(qrows.shape[0])
        ],
        axis=1,
    ).astype(jnp.bfloat16)
    k2_copy.wait()
    s2 = lax.dot_general(q_all[:, half:], k2buf[...], NT, preferred_element_type=jnp.float32)
    drain(gslot.at[pl.ds(0, heads - 1)], g_recv)
    for j in range(heads):
        grows[pl.ds(j * seqs, seqs), :] = gslot[j]
    ids = grows[...]
    sub_count = k2buf.shape[0]
    second = pick_lanes(s2, ids & (sub_count - 1))
    drain(kslot.at[pl.ds(0, devices - 1)], k_recv)
    k1 = kslot[...].astype(jnp.float32)
    k1 = k1.reshape(k1.shape[0] * k1.shape[1], half).astype(jnp.bfloat16)
    s1 = lax.dot_general(q_all[:, :half], k1, NT, preferred_element_type=jnp.float32)
    score = second + pick_lanes(s1, lax.shift_right_arithmetic(ids, log2(sub_count)))
    lane = lax.broadcasted_iota(jnp.int32, ids.shape, 1)
    mine = lax.shift_right_arithmetic(lane, log2(top)) == head_me
    best = jnp.max(jnp.where(mine, score, -jnp.inf), axis=1, keepdims=True)
    raised = jnp.where(mine, jnp.exp(jnp.where(mine, score - best, 0.0)), 0.0)
    weights = raised / jnp.sum(raised, axis=1, keepdims=True)
    weights = weights.astype(jnp.bfloat16).astype(jnp.float32)
    for j in range(heads):
        rolled[j] = pltpu.roll(weights, lax.rem(j - head_me + heads, heads) * top, 1)
    packed = rolled[0, pl.ds(0, seqs), :]
    for j in range(1, heads):
        packed = packed + rolled[j, pl.ds(j * seqs, seqs), :]
    wpack[...] = packed
    wslot[slot_me] = packed

    def send_weights(slot, where, head):
        pltpu.make_async_remote_copy(
            src_ref=wpack,
            dst_ref=wslot.at[slot_me],
            send_sem=w_send,
            recv_sem=w_recv,
            device_id=where,
            device_id_type=MESH,
        ).start()

    others(send_weights)
    high_count = rows // LANES
    all_seqs = devices * seqs
    high_iota = lax.broadcasted_iota(jnp.int32, (high_count, LANES), 0)
    low_iota = lax.broadcasted_iota(jnp.int32, (LANES, LANES), 0)
    base = dev_me * rows

    def high_hot(s, value):
        high = lax.shift_right_arithmetic(istage[pl.ds(s, 1), :] - base, 7)
        return jnp.where(high_iota == high, value, 0.0).astype(jnp.bfloat16)

    def low_hot(s):
        low = istage[pl.ds(s, 1), :] & (LANES - 1)
        return jnp.where(low_iota == low, 1.0, 0.0).astype(jnp.bfloat16)

    drain(islot.at[pl.ds(0, devices - 1)], i_recv)
    for slot in range(devices):
        istage[pl.ds(slot * seqs, seqs), :] = islot[slot]
    low_lane = lax.broadcasted_iota(jnp.int32, (LANES, LANES), 1).astype(jnp.float32)
    if early:

        def build(step, carry):
            some = istage[pl.ds(pl.multiple_of(step * 8, 8), 8), :] & (LANES - 1)
            some = some.astype(jnp.float32).T
            for u in range(8):
                hot = jnp.where(low_lane == some[:, u : u + 1], 1.0, 0.0)
                lows[step * 8 + u] = hot.astype(jnp.bfloat16)
            return carry

        lax.fori_loop(0, all_seqs // 8, build, 0)
    drain(wslot.at[pl.ds(0, devices - 1)], w_recv)
    for slot in range(devices):
        wstage[pl.ds(slot * seqs, seqs), :] = wslot[slot]
    span = groups * seqs
    lane = lax.broadcasted_iota(jnp.int32, (span, LANES), 1)
    block_of = lax.shift_right_arithmetic(lane, log2(top))
    for j in range(heads):
        total = jnp.zeros((span, LANES), jnp.float32)
        for h in range(heads):
            part = wstage[pl.ds(h * span, span), :]
            if h != j:
                part = pltpu.roll(part, (h - j) % heads * top, 1)
            total = jnp.where(block_of == h, part, total)
        wfin[pl.ds(j * span, span), :] = total

    pitch = all_seqs + 8

    def spread(step, carry):
        for u in range(32):
            s = step * 32 + u
            left = high_hot(s, wfin[pl.ds(s, 1), :])
            right = lows[s] if early else low_hot(s)
            wacc[pl.ds(s, high_count, stride=pitch), :] = lax.dot_general(
                left, right, NN if early else NT, preferred_element_type=jnp.float32
            )
        return carry

    lax.fori_loop(0, all_seqs // 32, spread, 0)

    def narrow(step, carry):
        wb[:, pl.ds(pl.multiple_of(step * LANES, LANES), LANES)] = wacc[
            pl.ds(pl.multiple_of(step * pitch, 8), all_seqs), :
        ].astype(jnp.bfloat16)
        return carry

    lax.fori_loop(0, high_count, narrow, 0, unroll=8)
    for copy in v_copies:
        copy.wait()

    piece = width // chunks
    half_slot = lax.div(head_me, 2) * groups + group_me

    def pass_on(c):
        drain(pair.at[c], a_recv.at[c])
        for i in range(heads // 2):
            both = accs[c, 2 * i + core_me] + pair[c, i]
            for g in range(groups):
                psend[c, i * groups + g] = both[g * seqs : (g + 1) * seqs, :].astype(jnp.bfloat16)
        pslot[c, half_slot] = psend[c, half_slot]

        def send_part(slot, where, head):
            pltpu.make_async_remote_copy(
                src_ref=psend.at[c, slot - lax.div(head + 1, 2) * groups],
                dst_ref=pslot.at[c, half_slot],
                send_sem=p_send.at[c],
                recv_sem=p_recv.at[c],
                device_id=where,
                device_id_type=MESH,
            ).start()

        others(send_part, 2)

    for c in range(chunks):
        acc = jnp.dot(
            wb[...], vbuf[:, pl.ds(c * piece, piece)], preferred_element_type=jnp.float32
        )
        for j in range(heads):
            accs[c, j] = acc[j * span : (j + 1) * span, :]
        for i in range(heads // 2):
            pltpu.make_async_remote_copy(
                src_ref=accs.at[c, 2 * i + 1 - core_me],
                dst_ref=pair.at[c, i],
                send_sem=a_send.at[c],
                recv_sem=a_recv.at[c],
                device_id=(t_me + 1 - 2 * core_me, b_me),
                device_id_type=MESH,
            ).start()
        if c > 0:
            pass_on(c - 1)
    pass_on(chunks - 1)

    for c in range(chunks):
        drain(pslot.at[c, pl.ds(0, devices // 2 - 1)], p_recv.at[c])
        total = jnp.zeros((seqs, piece), jnp.float32)
        for slot in range(devices // 2):
            total = total + pslot[c, slot].astype(jnp.float32)
        out_ref[:, pl.ds(c * piece, piece)] = total.astype(jnp.bfloat16)

    drain(qslot.at[pl.ds(0, heads - 1)], q_send)
    drain(gslot.at[pl.ds(0, heads - 1)], g_send)
    drain(kslot.at[pl.ds(0, devices - 1)], k_send)
    drain(islot.at[pl.ds(0, devices - 1)], i_send)
    drain(wslot.at[pl.ds(0, devices - 1)], w_send)
    for c in range(chunks):
        drain(pslot.at[c, pl.ds(0, devices // 2 - 1)], p_send.at[c])
        drain(pair.at[c], a_send.at[c])


def shards(nt, nb, queries, indices, first_keys, second_keys, values):
    seqs, heads, top = indices.shape
    width_q = queries.shape[2]
    half = width_q // 2
    firsts = first_keys.shape[1]
    sub_count = second_keys.shape[1]
    rows, width = values.shape
    devices = nt * nb
    all_seqs = devices * seqs
    assert heads * top == LANES and nt % heads == 0 and heads % 2 == 0
    chunks, pieces = 2, 4
    early = all_seqs <= 256
    vmem = pl.BlockSpec(memory_space=pltpu.VMEM)
    hbm = pl.BlockSpec(memory_space=pl.ANY)
    dma = pltpu.SemaphoreType.DMA
    return pl.pallas_call(
        functools.partial(kernel, (nt, nb, heads, seqs, top, chunks, pieces, early)),
        out_shape=jax.ShapeDtypeStruct((seqs, width), jnp.bfloat16),
        in_specs=[vmem, vmem, vmem, hbm, hbm],
        out_specs=vmem,
        scratch_shapes=[
            pltpu.VMEM((rows, width), jnp.bfloat16),
            pltpu.VMEM((sub_count, half), jnp.bfloat16),
            pltpu.VMEM((devices, firsts, half), jnp.bfloat16),
            pltpu.VMEM((devices, seqs, LANES), jnp.int32),
            pltpu.VMEM((heads, seqs, LANES), jnp.int32),
            pltpu.VMEM((seqs, LANES), jnp.int32),
            pltpu.VMEM((heads, seqs, heads, width_q), jnp.bfloat16),
            pltpu.VMEM((width_q // LANES, heads * seqs * heads, LANES), jnp.float32),
            pltpu.VMEM((heads * seqs, LANES), jnp.int32),
            pltpu.VMEM((heads, heads * seqs, LANES), jnp.float32),
            pltpu.VMEM((seqs, LANES), jnp.float32),
            pltpu.VMEM((devices, seqs, LANES), jnp.float32),
            pltpu.VMEM((all_seqs, LANES), jnp.int32),
            pltpu.VMEM((all_seqs, LANES), jnp.float32),
            pltpu.VMEM((all_seqs, LANES), jnp.float32),
            pltpu.VMEM((rows // LANES * (all_seqs + 8), LANES), jnp.float32),
            pltpu.VMEM((all_seqs, rows), jnp.bfloat16),
            pltpu.VMEM((all_seqs if early else 1, LANES, LANES), jnp.bfloat16),
            pltpu.VMEM((chunks, heads, all_seqs // heads, width // chunks), jnp.float32),
            pltpu.VMEM((chunks, heads // 2, all_seqs // heads, width // chunks), jnp.float32),
            pltpu.VMEM((chunks, devices // 2, seqs, width // chunks), jnp.bfloat16),
            pltpu.VMEM((chunks, devices // 2, seqs, width // chunks), jnp.bfloat16),
            dma((pieces,)),
            dma,
            dma,
            dma,
            dma,
            dma,
            dma,
            dma,
            dma,
            dma,
            dma,
            dma,
            dma,
            dma,
            dma((chunks,)),
            dma((chunks,)),
            dma((chunks,)),
            dma((chunks,)),
        ],
        compiler_params=pltpu.CompilerParams(
            collective_id=0, has_side_effects=True, vmem_limit_bytes=60 * 1024 * 1024
        ),
    )(queries, indices, first_keys, second_keys, values)


def solution(mesh):
    placed = (
        P(("table", "batch"), None, None),
        P(("table", "batch"), None, None),
        P(None, ("table", "batch"), None),
        P(),
        P(("table", "batch"), None),
    )
    body = functools.partial(shards, mesh.shape["table"], mesh.shape["batch"])
    return jax.shard_map(
        body, mesh=mesh, in_specs=placed, out_specs=P(("table", "batch"), None), check_vma=False
    )
```

```python
import functools

import jax
import jax.numpy as jnp
from jax import lax
from jax.experimental import pallas as pl
from jax.experimental.pallas import tpu as pltpu
from jax.sharding import PartitionSpec as P

MESH = pl.DeviceIdType.MESH
LANES = 128
NT = (((1,), (1,)), ((), ()))
NN = (((1,), (0,)), ((), ()))


def log2(number):
    assert number & (number - 1) == 0
    return number.bit_length() - 1


def pick_lanes(table, ids):
    picked = jnp.zeros(ids.shape, jnp.float32)
    inner = ids & (LANES - 1)
    outer = lax.shift_right_arithmetic(ids, 7)
    for part in range(table.shape[1] // LANES):
        got = jnp.take_along_axis(table[:, part * LANES : (part + 1) * LANES], inner, axis=1)
        picked = jnp.where(outer == part, got, picked)
    return picked


def kernel(
    shape,
    q_ref,
    i_ref,
    fk_ref,
    sk_ref,
    v_ref,
    out_ref,
    vbuf,
    k2buf,
    kslot,
    islot,
    gslot,
    icomp,
    qslot,
    qrows,
    grows,
    rolled,
    wpack,
    wslot,
    istage,
    wstage,
    wfin,
    wacc,
    wb,
    lows,
    accs,
    pair,
    psend,
    pslot,
    v_sem,
    k2_sem,
    k_send,
    k_recv,
    i_send,
    i_recv,
    r_send,
    r_recv,
    g_send,
    g_recv,
    q_send,
    q_recv,
    w_send,
    w_recv,
    a_send,
    a_recv,
    p_send,
    p_recv,
):
    nt, nb, heads, seqs, top, chunks, pieces, early = shape
    devices = nt * nb
    groups = devices // heads
    half = q_ref.shape[2] // 2
    rows, width = v_ref.shape
    t_me, b_me = lax.axis_index("table"), lax.axis_index("batch")
    dev_me = t_me * nb + b_me
    core_me = lax.rem(t_me, 2)
    head_me = lax.rem(t_me, heads)
    group_me = lax.div(t_me, heads) * nb + b_me
    slot_me = head_me * groups + group_me

    def flips(x, count):
        bits = [(x // 2**i) % 2 for i in range(log2(count))]
        return [
            x + sum((1 - 2 * bit) * 2**i for i, bit in enumerate(bits) if mask >> i & 1)
            for mask in range(count)
        ]

    t_flips, b_flips = flips(t_me, nt), flips(b_me, nb)
    t_heads = [lax.rem(t, heads) for t in t_flips]
    t_slots = [h * groups + lax.div(t, heads) * nb for t, h in zip(t_flips, t_heads)]
    masks = sorted(
        ((mt, mb) for mt in range(nt) for mb in range(nb) if mt or mb),
        key=lambda m: (m[1] + bin(m[0] >> 1).count("1"), m),
        reverse=True,
    )

    def others(body, stride=1):
        for mt, mb in masks:
            if mt % stride == 0:
                body(t_slots[mt] + b_flips[mb], (t_flips[mt], b_flips[mb]), t_heads[mt])

    def drain(ref, sem):
        pltpu.make_async_copy(ref, ref, sem).wait()

    barrier = pltpu.get_barrier_semaphore()
    others(
        lambda slot, where, head: pl.semaphore_signal(
            barrier, inc=1, device_id=where, device_id_type=MESH
        )
    )
    k2_copy = pltpu.make_async_copy(sk_ref.at[head_me], k2buf, k2_sem)
    k2_copy.start()
    block = rows // pieces
    v_copies = [
        pltpu.make_async_copy(
            v_ref.at[pl.ds(p * block, block)], vbuf.at[pl.ds(p * block, block)], v_sem.at[p]
        )
        for p in range(pieces)
    ]
    for copy in v_copies:
        copy.start()

    for h in range(heads):
        for s in range(seqs):
            icomp[pl.ds(s, 1), pl.ds(h * top, top)] = i_ref[s, pl.ds(h, 1), :]
    islot[slot_me] = icomp[...]
    kslot[dev_me] = fk_ref[head_me]
    gslot[head_me] = icomp[...]
    qslot[head_me] = q_ref[...]
    pl.semaphore_wait(barrier, devices - 1)

    def send_q(j):
        other = lax.rem(head_me + j, heads)
        pltpu.make_async_remote_copy(
            src_ref=q_ref,
            dst_ref=qslot.at[head_me],
            send_sem=q_send,
            recv_sem=q_recv,
            device_id=(lax.div(t_me, heads) * heads + other, b_me),
            device_id_type=MESH,
        ).start()

    def send_group_ids(j):
        other = lax.rem(head_me + j, heads)
        pltpu.make_async_remote_copy(
            src_ref=icomp,
            dst_ref=gslot.at[head_me],
            send_sem=g_send,
            recv_sem=g_recv,
            device_id=(lax.div(t_me, heads) * heads + other, b_me),
            device_id_type=MESH,
        ).start()

    def send_keys(slot, where, head):
        pltpu.make_async_remote_copy(
            src_ref=fk_ref.at[head],
            dst_ref=kslot.at[dev_me],
            send_sem=k_send,
            recv_sem=k_recv,
            device_id=where,
            device_id_type=MESH,
        ).start()

    def send_ids(slot, where, head):
        pltpu.make_async_remote_copy(
            src_ref=icomp,
            dst_ref=islot.at[slot_me],
            send_sem=i_send,
            recv_sem=i_recv,
            device_id=where,
            device_id_type=MESH,
        ).start()

    others(send_keys)
    for j in range(1, heads):
        send_q(j)
        send_group_ids(j)
    others(send_ids)

    drain(qslot.at[pl.ds(0, heads - 1)], q_recv)
    for j in range(heads):
        for s in range(seqs):
            one = qslot[j, s].astype(jnp.float32)
            for c in range(qrows.shape[0]):
                qrows[c, pl.ds((j * seqs + s) * heads, heads), :] = one[
                    :, c * LANES : (c + 1) * LANES
                ]
    q_all = jnp.concatenate(
        [
            qrows.at[c][pl.ds(head_me, heads * seqs, stride=heads), :]
            for c in range(qrows.shape[0])
        ],
        axis=1,
    ).astype(jnp.bfloat16)
    k2_copy.wait()
    s2 = lax.dot_general(q_all[:, half:], k2buf[...], NT, preferred_element_type=jnp.float32)
    drain(gslot.at[pl.ds(0, heads - 1)], g_recv)
    for j in range(heads):
        grows[pl.ds(j * seqs, seqs), :] = gslot[j]
    ids = grows[...]
    sub_count = k2buf.shape[0]
    second = pick_lanes(s2, ids & (sub_count - 1))
    drain(kslot.at[pl.ds(0, devices - 1)], k_recv)
    k1 = kslot[...].astype(jnp.float32)
    k1 = k1.reshape(k1.shape[0] * k1.shape[1], half).astype(jnp.bfloat16)
    s1 = lax.dot_general(q_all[:, :half], k1, NT, preferred_element_type=jnp.float32)
    score = second + pick_lanes(s1, lax.shift_right_arithmetic(ids, log2(sub_count)))
    lane = lax.broadcasted_iota(jnp.int32, ids.shape, 1)
    mine = lax.shift_right_arithmetic(lane, log2(top)) == head_me
    best = jnp.max(jnp.where(mine, score, -jnp.inf), axis=1, keepdims=True)
    raised = jnp.where(mine, jnp.exp(jnp.where(mine, score - best, 0.0)), 0.0)
    weights = raised / jnp.sum(raised, axis=1, keepdims=True)
    weights = weights.astype(jnp.bfloat16).astype(jnp.float32)
    for j in range(heads):
        rolled[j] = pltpu.roll(weights, lax.rem(j - head_me + heads, heads) * top, 1)
    packed = rolled[0, pl.ds(0, seqs), :]
    for j in range(1, heads):
        packed = packed + rolled[j, pl.ds(j * seqs, seqs), :]
    wpack[...] = packed
    wslot[slot_me] = packed

    def send_weights(slot, where, head):
        pltpu.make_async_remote_copy(
            src_ref=wpack,
            dst_ref=wslot.at[slot_me],
            send_sem=w_send,
            recv_sem=w_recv,
            device_id=where,
            device_id_type=MESH,
        ).start()

    others(send_weights)
    high_count = rows // LANES
    all_seqs = devices * seqs
    high_iota = lax.broadcasted_iota(jnp.int32, (high_count, LANES), 0)
    low_iota = lax.broadcasted_iota(jnp.int32, (LANES, LANES), 0)
    base = dev_me * rows

    def high_hot(s, value):
        high = lax.shift_right_arithmetic(istage[pl.ds(s, 1), :] - base, 7)
        return jnp.where(high_iota == high, value, 0.0).astype(jnp.bfloat16)

    def low_hot(s):
        low = istage[pl.ds(s, 1), :] & (LANES - 1)
        return jnp.where(low_iota == low, 1.0, 0.0).astype(jnp.bfloat16)

    drain(islot.at[pl.ds(0, devices - 1)], i_recv)
    for slot in range(devices):
        istage[pl.ds(slot * seqs, seqs), :] = islot[slot]
    low_lane = lax.broadcasted_iota(jnp.int32, (LANES, LANES), 1).astype(jnp.float32)
    if early:

        def build(step, carry):
            some = istage[pl.ds(pl.multiple_of(step * 8, 8), 8), :] & (LANES - 1)
            some = some.astype(jnp.float32).T
            for u in range(8):
                hot = jnp.where(low_lane == some[:, u : u + 1], 1.0, 0.0)
                lows[step * 8 + u] = hot.astype(jnp.bfloat16)
            return carry

        lax.fori_loop(0, all_seqs // 8, build, 0)
    drain(wslot.at[pl.ds(0, devices - 1)], w_recv)
    for slot in range(devices):
        wstage[pl.ds(slot * seqs, seqs), :] = wslot[slot]
    span = groups * seqs
    lane = lax.broadcasted_iota(jnp.int32, (span, LANES), 1)
    block_of = lax.shift_right_arithmetic(lane, log2(top))
    for j in range(heads):
        total = jnp.zeros((span, LANES), jnp.float32)
        for h in range(heads):
            part = wstage[pl.ds(h * span, span), :]
            if h != j:
                part = pltpu.roll(part, (h - j) % heads * top, 1)
            total = jnp.where(block_of == h, part, total)
        wfin[pl.ds(j * span, span), :] = total

    pitch = all_seqs + 8
    burst = min(all_seqs, LANES)

    def spread(step, carry):
        for u in range(burst):
            s = step * burst + u
            left = high_hot(s, wfin[pl.ds(s, 1), :])
            right = lows[s] if early else low_hot(s)
            wacc[pl.ds(s, high_count, stride=pitch), :] = lax.dot_general(
                left, right, NN if early else NT, preferred_element_type=jnp.float32
            )
        return carry

    lax.fori_loop(0, all_seqs // burst, spread, 0)

    def narrow(step, carry):
        wb[:, pl.ds(pl.multiple_of(step * LANES, LANES), LANES)] = wacc[
            pl.ds(pl.multiple_of(step * pitch, 8), all_seqs), :
        ].astype(jnp.bfloat16)
        return carry

    lax.fori_loop(0, high_count, narrow, 0, unroll=8)
    for copy in v_copies:
        copy.wait()

    piece = width // chunks
    half_slot = lax.div(head_me, 2) * groups + group_me

    def pass_on(c):
        drain(pair.at[c], a_recv.at[c])
        for i in range(heads // 2):
            both = accs[c, 2 * i + core_me] + pair[c, i]
            for g in range(groups):
                psend[c, i * groups + g] = both[g * seqs : (g + 1) * seqs, :].astype(jnp.bfloat16)
        pslot[c, half_slot] = psend[c, half_slot]

        def send_part(slot, where, head):
            pltpu.make_async_remote_copy(
                src_ref=psend.at[c, slot - lax.div(head + 1, 2) * groups],
                dst_ref=pslot.at[c, half_slot],
                send_sem=p_send.at[c],
                recv_sem=p_recv.at[c],
                device_id=where,
                device_id_type=MESH,
            ).start()

        others(send_part, 2)

    for c in range(chunks):
        acc = jnp.dot(
            wb[...], vbuf[:, pl.ds(c * piece, piece)], preferred_element_type=jnp.float32
        )
        for j in range(heads):
            accs[c, j] = acc[j * span : (j + 1) * span, :]
        for i in range(heads // 2):
            pltpu.make_async_remote_copy(
                src_ref=accs.at[c, 2 * i + 1 - core_me],
                dst_ref=pair.at[c, i],
                send_sem=a_send.at[c],
                recv_sem=a_recv.at[c],
                device_id=(t_me + 1 - 2 * core_me, b_me),
                device_id_type=MESH,
            ).start()
        if c > 0:
            pass_on(c - 1)
    pass_on(chunks - 1)

    for c in range(chunks):
        drain(pslot.at[c, pl.ds(0, devices // 2 - 1)], p_recv.at[c])
        total = jnp.zeros((seqs, piece), jnp.float32)
        for slot in range(devices // 2):
            total = total + pslot[c, slot].astype(jnp.float32)
        out_ref[:, pl.ds(c * piece, piece)] = total.astype(jnp.bfloat16)

    drain(qslot.at[pl.ds(0, heads - 1)], q_send)
    drain(gslot.at[pl.ds(0, heads - 1)], g_send)
    drain(kslot.at[pl.ds(0, devices - 1)], k_send)
    drain(islot.at[pl.ds(0, devices - 1)], i_send)
    drain(wslot.at[pl.ds(0, devices - 1)], w_send)
    for c in range(chunks):
        drain(pslot.at[c, pl.ds(0, devices // 2 - 1)], p_send.at[c])
        drain(pair.at[c], a_send.at[c])


def shards(nt, nb, queries, indices, first_keys, second_keys, values):
    seqs, heads, top = indices.shape
    width_q = queries.shape[2]
    half = width_q // 2
    firsts = first_keys.shape[1]
    sub_count = second_keys.shape[1]
    rows, width = values.shape
    devices = nt * nb
    all_seqs = devices * seqs
    assert heads * top == LANES and nt % heads == 0 and heads % 2 == 0
    chunks, pieces = 2, 4
    early = all_seqs <= 256
    vmem = pl.BlockSpec(memory_space=pltpu.VMEM)
    hbm = pl.BlockSpec(memory_space=pl.ANY)
    dma = pltpu.SemaphoreType.DMA
    return pl.pallas_call(
        functools.partial(kernel, (nt, nb, heads, seqs, top, chunks, pieces, early)),
        out_shape=jax.ShapeDtypeStruct((seqs, width), jnp.bfloat16),
        in_specs=[vmem, vmem, vmem, hbm, hbm],
        out_specs=vmem,
        scratch_shapes=[
            pltpu.VMEM((rows, width), jnp.bfloat16),
            pltpu.VMEM((sub_count, half), jnp.bfloat16),
            pltpu.VMEM((devices, firsts, half), jnp.bfloat16),
            pltpu.VMEM((devices, seqs, LANES), jnp.int32),
            pltpu.VMEM((heads, seqs, LANES), jnp.int32),
            pltpu.VMEM((seqs, LANES), jnp.int32),
            pltpu.VMEM((heads, seqs, heads, width_q), jnp.bfloat16),
            pltpu.VMEM((width_q // LANES, heads * seqs * heads, LANES), jnp.float32),
            pltpu.VMEM((heads * seqs, LANES), jnp.int32),
            pltpu.VMEM((heads, heads * seqs, LANES), jnp.float32),
            pltpu.VMEM((seqs, LANES), jnp.float32),
            pltpu.VMEM((devices, seqs, LANES), jnp.float32),
            pltpu.VMEM((all_seqs, LANES), jnp.int32),
            pltpu.VMEM((all_seqs, LANES), jnp.float32),
            pltpu.VMEM((all_seqs, LANES), jnp.float32),
            pltpu.VMEM((rows // LANES * (all_seqs + 8), LANES), jnp.float32),
            pltpu.VMEM((all_seqs, rows), jnp.bfloat16),
            pltpu.VMEM((all_seqs if early else 1, LANES, LANES), jnp.bfloat16),
            pltpu.VMEM((chunks, heads, all_seqs // heads, width // chunks), jnp.float32),
            pltpu.VMEM((chunks, heads // 2, all_seqs // heads, width // chunks), jnp.float32),
            pltpu.VMEM((chunks, devices // 2, seqs, width // chunks), jnp.bfloat16),
            pltpu.VMEM((chunks, devices // 2, seqs, width // chunks), jnp.bfloat16),
            dma((pieces,)),
            dma,
            dma,
            dma,
            dma,
            dma,
            dma,
            dma,
            dma,
            dma,
            dma,
            dma,
            dma,
            dma,
            dma((chunks,)),
            dma((chunks,)),
            dma((chunks,)),
            dma((chunks,)),
        ],
        compiler_params=pltpu.CompilerParams(
            collective_id=0, has_side_effects=True, vmem_limit_bytes=60 * 1024 * 1024
        ),
    )(queries, indices, first_keys, second_keys, values)


def solution(mesh):
    placed = (
        P(("table", "batch"), None, None),
        P(("table", "batch"), None, None),
        P(None, ("table", "batch"), None),
        P(),
        P(("table", "batch"), None),
    )
    body = functools.partial(shards, mesh.shape["table"], mesh.shape["batch"])
    return jax.shard_map(
        body, mesh=mesh, in_specs=placed, out_specs=P(("table", "batch"), None), check_vma=False
    )
```
